128 devices in a mesh: bngroup: 8 (over z, core), rep: 16 (over x, y).
Axes of the slice: x: 4, y: 4, z: 4, core: 2. Of those that a mesh axis runs over, the one named last changes fastest.
Arguments:
- images: bfloat16 [1536, 7, 7, 2048], P(('bngroup', 'rep')), may hold values from -12 to 12
- cotangent: bfloat16 [1536, 7, 7, 2048], P(('bngroup', 'rep')), may hold values from -6 to 6
- w_reduce: bfloat16 [2048, 512], replicated, may hold values from -0.125 to 0.125
- w_spatial: bfloat16 [4608, 512], replicated, may hold values from -0.09375 to 0.09375
- w_expand: bfloat16 [2048, 512], replicated, may hold values from -0.25 to 0.25
- norm_gain: float32 [3072], replicated, may hold values from 0.25 to 1.75
- norm_shift: float32 [3072], replicated, may hold values from -3 to 3
Outputs:
- output: bfloat16 [1536, 7, 7, 2048], P(('bngroup', 'rep'))
- in_grad: bfloat16 [1536, 7, 7, 2048], P(('bngroup', 'rep'))
- weight_grads: float32 [8704, 512], P('bngroup', 'rep')
- norm_grads: float32 [2, 3072], replicated
The draws below stay inside these ranges and needn't reach their ends.
All inputs are finite; a program needn't handle non-finite values.
Results may differ from the reference program's by a relative error of at most 0.007.
Values sent between devices are 32-bit elements.
No kernel may reach another device: no remote copies, remote signals or barrier semaphores. Data moves between devices by JAX's collectives and lax.ppermute only.
A program may use at most 192 MiB of HBM per device.

```python
import jax
import jax.numpy as jnp
from jax import lax

WIDE = 2048
MID = 512
SIDE = 7
IMG_DEV = 12
IMAGES = 1536
NORM_CH = 3072
N_BNGROUP = 8
N_REP = 16


def draw_images(key, part):
    base_key, scale_key = jax.random.split(jax.random.fold_in(key, 11))
    values = jnp.clip(jax.random.normal(base_key, (IMAGES, SIDE, SIDE, WIDE), jnp.float32), -6.0, 6.0)
    scales = jnp.exp(jax.random.uniform(scale_key, (IMAGES, 1, 1, 1), jnp.float32, -0.69, 0.69))
    return (values * scales).astype(jnp.bfloat16)


def block_scale(stream_key, shape, shards, smallest, high):
    factor_of, own = 1.0, jax.random.fold_in(stream_key, 6)
    for axis_at, shards_of in shards:
        draws = jnp.exp(jax.random.uniform(jax.random.fold_in(own, axis_at), (shards_of,), jnp.float32, smallest / len(shards), high / len(shards)))
        factor_of = factor_of * jnp.repeat(draws, shape[axis_at] // shards_of).reshape([-1 if axis == axis_at else 1 for axis in range(len(shape))])
    return factor_of


def bell_draw(stream_key, extent, scale, bound, shards=(), kind=jnp.bfloat16):
    values = jax.random.normal(stream_key, extent, jnp.float32) * scale
    if len(shards) > 0:
        values = block_scale(stream_key, extent, shards, -0.22, 0.18) * values
    return jnp.clip(values, min=-bound, max=bound).astype(kind)


def setup_inputs(seed: int = 0) -> dict:
    seeds = jax.random.split(jax.random.key(seed), 8)
    return {
        "images": draw_images(jax.random.fold_in(seeds[7], 71), 0),
        "cotangent": bell_draw(seeds[1], (IMAGES, SIDE, SIDE, WIDE), 1.0, 6.0, ((0, 128),)),
        "w_reduce": bell_draw(seeds[2], (WIDE, MID), WIDE ** -0.5, 0.125),
        "w_spatial": bell_draw(seeds[3], (9 * MID, MID), (9 * MID) ** -0.5, 0.09375),
        "w_expand": bell_draw(seeds[4], (WIDE, MID), MID ** -0.5, 0.25),
        "norm_gain": jnp.clip(1.0 + 0.15 * jax.random.normal(seeds[5], (NORM_CH,), jnp.float32), 0.25, 1.75),
        "norm_shift": bell_draw(seeds[6], (NORM_CH,), 0.5, 3.0, (), jnp.float32),
    }


EPS = 0.25

def matmul(left, right):
    return jnp.dot(left, right, preferred_element_type=jnp.float32)

def contract(left, right, left_dim, right_dim):
    return lax.dot_general(left, right, (((left_dim,), (right_dim,)), ((), ())), preferred_element_type=jnp.float32)

def slope(value):
    sigma = jax.nn.sigmoid(value)
    return sigma * (1.0 + value * (1.0 - sigma))

def normalize(pre_norm, norm_gain, norm_shift):
    centre = lax.optimization_barrier(jnp.mean(pre_norm, axis=0))
    spread = lax.optimization_barrier(jnp.mean(jnp.square(pre_norm - centre), axis=0))
    inverse = lax.rsqrt(spread + EPS)
    scaled = (pre_norm - centre) * inverse
    return (scaled, inverse, norm_gain * scaled + norm_shift)

def norm_back(upstream, scaled, inverse, norm_gain):
    shift_sum = lax.optimization_barrier(jnp.sum(upstream, axis=0))
    gain_sum = lax.optimization_barrier(jnp.sum(upstream * scaled, axis=0))
    number = upstream.shape[0]
    result = norm_gain * inverse * (upstream - shift_sum / number - scaled * gain_sum / number)
    return (result.astype(jnp.bfloat16), shift_sum, gain_sum)

def unfold(field):
    length = field.shape[1]
    padded = jnp.pad(field, ((0, 0), (1, 1), (1, 1), (0, 0)))
    windows = [padded[:, row_tap:row_tap + length, col_tap:col_tap + length, :] for row_tap in range(3) for col_tap in range(3)]
    return jnp.concatenate(windows, axis=-1).reshape(-1, 9 * field.shape[3])

def fold_back(columns, images_count, length, channels):
    shaped = columns.reshape(images_count, length, length, 9, channels)
    summed = jnp.zeros((images_count, length + 2, length + 2, channels), jnp.float32)
    for row_tap in range(3):
        for col_tap in range(3):
            summed = summed + jnp.pad(shaped[:, :, :, 3 * row_tap + col_tap, :], ((0, 0), (row_tap, 2 - row_tap), (col_tap, 2 - col_tap), (0, 0)))
    return summed[:, 1:length + 1, 1:length + 1, :].reshape(-1, channels)

def block_pass(images, cotangent, w_reduce, w_spatial, w_expand, norm_gain, norm_shift):
    images_count = images.shape[0]
    length = images.shape[1]
    wide_ch = images.shape[3]
    mid_ch = w_reduce.shape[1]
    flat_in = images.reshape(-1, wide_ch)
    gain_one, gain_two, gain_three = (norm_gain[:mid_ch], norm_gain[mid_ch:2 * mid_ch], norm_gain[2 * mid_ch:])
    shift_one, shift_two, shift_three = (norm_shift[:mid_ch], norm_shift[mid_ch:2 * mid_ch], norm_shift[2 * mid_ch:])
    scaled_one, inverse_one, normed_one = normalize(matmul(flat_in, w_reduce), gain_one, shift_one)
    hidden_one = jax.nn.silu(normed_one).astype(jnp.bfloat16)
    patches = unfold(hidden_one.reshape(images_count, length, length, mid_ch))
    scaled_two, inverse_two, normed_two = normalize(matmul(patches, w_spatial), gain_two, shift_two)
    hidden_two = jax.nn.silu(normed_two).astype(jnp.bfloat16)
    scaled_three, inverse_three, normed_three = normalize(contract(hidden_two, w_expand, 1, 1), gain_three, shift_three)
    summed_in = normed_three + flat_in.astype(jnp.float32)
    output = jax.nn.silu(summed_in).astype(jnp.bfloat16)
    upstream = cotangent.reshape(-1, wide_ch).astype(jnp.float32) * slope(summed_in)
    grad_three, shift_sum_three, gain_sum_three = norm_back(upstream, scaled_three, inverse_three, gain_three)
    back_two = matmul(grad_three, w_expand) * slope(normed_two)
    grad_two, shift_sum_two, gain_sum_two = norm_back(back_two, scaled_two, inverse_two, gain_two)
    back_one = fold_back(contract(grad_two, w_spatial, 1, 1), images_count, length, mid_ch) * slope(normed_one)
    grad_one, shift_sum_one, gain_sum_one = norm_back(back_one, scaled_one, inverse_one, gain_one)
    in_grad = (upstream + contract(grad_one, w_reduce, 1, 1)).astype(jnp.bfloat16)
    weight_grads = jnp.concatenate([contract(flat_in, grad_one, 0, 0), contract(patches, grad_two, 0, 0), contract(grad_three, hidden_two, 0, 0)], axis=0)
    norm_grads = jnp.stack([jnp.concatenate([gain_sum_one, gain_sum_two, gain_sum_three]), jnp.concatenate([shift_sum_one, shift_sum_two, shift_sum_three])])
    return (output.reshape(images.shape), in_grad.reshape(images.shape), weight_grads, norm_grads)

def reference(images, cotangent, w_reduce, w_spatial, w_expand, norm_gain, norm_shift):

    def regroup(array):
        tail = array.shape[1:]
        return array.reshape((N_BNGROUP, N_REP, IMG_DEV) + tail).swapaxes(0, 1).reshape((N_REP, N_BNGROUP * IMG_DEV) + tail)

    def ungroup(array):
        tail = array.shape[2:]
        return array.reshape((N_REP, N_BNGROUP, IMG_DEV) + tail).swapaxes(0, 1).reshape((IMAGES,) + tail)

    def group_step(totals, group_items):
        output, in_grad, weight_part, norm_part = block_pass(group_items[0], group_items[1], w_reduce, w_spatial, w_expand, norm_gain, norm_shift)
        return ((totals[0] + weight_part, totals[1] + norm_part), (output, in_grad))
    start_totals = (jnp.zeros((2 * WIDE + 9 * MID, MID), jnp.float32), jnp.zeros((2, 2 * MID + WIDE), jnp.float32))
    totals, results = lax.scan(group_step, start_totals, (regroup(images), regroup(cotangent)))
    return (ungroup(results[0]), ungroup(results[1]), totals[0] / IMAGES, totals[1] / IMAGES)
```

```python
import functools

import jax
import jax.numpy as jnp
from jax import lax
from jax.experimental import pallas as pl
from jax.experimental.pallas import tpu as pltpu
from jax.sharding import Mesh
from jax.sharding import PartitionSpec as P

BNGROUP = ("bngroup_0", "bngroup_1")
REP = ("rep_0", "rep_1")
BNGROUP_REP = ("bngroup_0", "bngroup_1", "rep_0", "rep_1")
EPS = 0.25
F32 = jnp.float32
BF16 = jnp.bfloat16
MIB = 1 << 20
LANES = 128


def sigmoid(v):
    return 0.5 + 0.5 * jnp.tanh(0.5 * v)


def slope(v):
    s = sigmoid(v)
    return s * (1.0 + v * (1.0 - s))


def real_rows(rows):
    return (lax.broadcasted_iota(jnp.int32, (rows, 1), 0) & 7) != 7


def unpack(stat_ref, first, count):
    total = jnp.sum(stat_ref[:, first : first + count, :], axis=0)
    return jnp.concatenate([total[k : k + 1, :] for k in range(count)], axis=1)


def pack(out_ref, first, row):
    count = row.shape[1] // LANES
    rows = jnp.concatenate([row[:, k * LANES : (k + 1) * LANES] for k in range(count)], axis=0)
    out_ref[:, first : first + count, :] = jnp.broadcast_to(
        rows[None], (out_ref.shape[0], count, LANES)
    )


def moments(stat_ref, first, count, number):
    centre = unpack(stat_ref, first, count) / number
    second = unpack(stat_ref, first + count, count) / number
    spread = jnp.maximum(second - centre * centre, 0.0)
    return centre, lax.rsqrt(spread + EPS)


def column_sum(v):
    return jnp.sum(v, axis=0, keepdims=True)


def call(kernel, grid, in_specs, out_specs, out_shape, flops, vmem, scratch=(), prefetch=0):
    return pl.pallas_call(
        kernel,
        grid_spec=pltpu.PrefetchScalarGridSpec(
            num_scalar_prefetch=prefetch,
            grid=grid,
            in_specs=in_specs,
            out_specs=out_specs,
            scratch_shapes=list(scratch),
        ),
        out_shape=out_shape,
        compiler_params=pltpu.CompilerParams(
            dimension_semantics=("arbitrary",) * len(grid), vmem_limit_bytes=vmem * MIB
        ),
        cost_estimate=pl.CostEstimate(flops=flops, bytes_accessed=flops // 400, transcendentals=0),
    )


def whole(shape):
    return pl.BlockSpec(shape, lambda *_: (0,) * len(shape))


def reduce_kernel(x_ref, w_ref, pre_ref, xp_ref, stat_ref, sums):
    step = pl.program_id(0)
    rows = pre_ref.shape[0]
    x = x_ref[...].astype(F32).reshape(rows, x_ref.shape[3])
    x = jnp.where(real_rows(rows), x, 0.0).astype(BF16)
    xp_ref[...] = x
    p = jnp.dot(x, w_ref[...], preferred_element_type=F32)
    pre_ref[...] = p

    @pl.when(step == 0)
    def _():
        sums[...] = jnp.zeros_like(sums)

    sums[0:1, :] += column_sum(p)
    sums[1:2, :] += column_sum(p * p)

    @pl.when(step == pl.num_programs(0) - 1)
    def _():
        pack(stat_ref, 0, sums[0:1, :])
        pack(stat_ref, 4, sums[1:2, :])


def fill_shifted(shifted, field):
    images, _, _, channels = shifted.shape[1:]
    zero = jnp.zeros((images, 1, 8, channels), F32)
    rows = field.shape[0]
    for k, moved in enumerate((pltpu.roll(field, 1, 0), field, pltpu.roll(field, rows - 1, 0))):
        shifted[k, :, 1:8] = moved.reshape(images, 7, 8, channels)
        shifted[k, :, 0:1] = zero
        shifted[k, :, 8:9] = zero


def conv_kernel(number, pre1_ref, stat1_ref, gs_ref, w_ref, patch_ref, pre2_ref, stat_ref, shifted):
    step = pl.program_id(0)
    rows = pre2_ref.shape[0]

    @pl.when(step == 0)
    def _():
        centre, inverse = moments(stat1_ref, 0, 4, number)
        v = gs_ref[0:1, :] * ((pre1_ref[...] - centre) * inverse) + gs_ref[1:2, :]
        fill_shifted(shifted, jnp.where(real_rows(rows), v * sigmoid(v), 0.0))

    piece = shifted[lax.rem(step, 3), :, pl.ds(lax.div(step, 3), 7)]
    piece = piece.reshape(rows, piece.shape[3]).astype(BF16)
    patch_ref[...] = piece
    product = jnp.dot(piece, w_ref[...], preferred_element_type=F32)

    @pl.when(step == 0)
    def _():
        pre2_ref[...] = product

    @pl.when(step > 0)
    def _():
        pre2_ref[...] += product

    @pl.when(step == pl.num_programs(0) - 1)
    def _():
        p = jnp.where(real_rows(rows), pre2_ref[...], 0.0)
        pre2_ref[...] = p
        pack(stat_ref, 0, column_sum(p))
        pack(stat_ref, 4, column_sum(p * p))


def expand_kernel(number, pre2_ref, stat2_ref, gs_ref, w_ref, h2_ref, pre3_ref, stat_ref):
    rows = h2_ref.shape[0]

    @pl.when(pl.program_id(0) == 0)
    def _():
        centre, inverse = moments(stat2_ref, 0, 4, number)
        v = gs_ref[0:1, :] * ((pre2_ref[...] - centre) * inverse) + gs_ref[1:2, :]
        h2_ref[...] = jnp.where(real_rows(rows), v * sigmoid(v), 0.0).astype(BF16)

    p = lax.dot_general(
        h2_ref[...], w_ref[...], (((1,), (1,)), ((), ())), preferred_element_type=F32
    )
    pre3_ref[...] = p
    pack(stat_ref, 0, column_sum(p))
    pack(stat_ref, 4, column_sum(p * p))


def wide_moments(stat_ref, number):
    parts = [moments(stat_ref, 8 * k, 4, number) for k in range(stat_ref.shape[1] // 8)]
    return tuple(jnp.concatenate([p[i] for p in parts], axis=1) for i in range(2))


def out_kernel(number, pre3_ref, x_ref, ct_ref, stat3_ref, gs_ref, out_ref, up_ref, stat_ref, sums, rowsc):
    step = pl.program_id(0)
    images = x_ref.shape[0]

    @pl.when(step == 0)
    def _():
        centre, inverse = wide_moments(stat3_ref, number)
        rowsc[0:1, :] = centre
        rowsc[1:2, :] = inverse
        sums[...] = jnp.zeros_like(sums)

    width = 512
    real = lax.broadcasted_iota(jnp.int32, (8, width), 0) != 7
    for block in range(x_ref.shape[3] // width):
        cols = slice(block * width, (block + 1) * width)
        centre = rowsc[0:1, cols]
        inverse = rowsc[1:2, cols]
        gain = gs_ref[0:1, cols]
        shift = gs_ref[1:2, cols]

        def group(g, carry, cols=cols, centre=centre, inverse=inverse, gain=gain, shift=shift):
            first, second = carry
            image = lax.div(g, 7)
            line = lax.rem(g, 7)
            at = pl.ds(pl.multiple_of(g * 8, 8), 8)
            scaled = (pre3_ref[at, cols] - centre) * inverse
            v = gain * scaled + shift + x_ref[image, line, :, cols].astype(F32)
            s = sigmoid(v)
            out = v * s
            out_ref[image, line, :, cols] = out.astype(BF16)
            up = ct_ref[image, line, :, cols].astype(F32) * (s * (1.0 + (v - out)))
            up = jnp.where(real, up, 0.0)
            up_ref[at, cols] = up
            return first + up, second + up * scaled

        zero = jnp.zeros((8, width), F32)
        first, second = lax.fori_loop(0, images * 7, group, (zero, zero), unroll=4)
        sums[0:8, cols] += first
        sums[8:16, cols] += second

    @pl.when(step == pl.num_programs(0) - 1)
    def _():
        for k in range(stat_ref.shape[1] // 8):
            cols = slice(512 * k, 512 * (k + 1))
            pack(stat_ref, 8 * k, column_sum(sums[0:8, cols]))
            pack(stat_ref, 8 * k + 4, column_sum(sums[8:16, cols]))


def back_two_kernel(number, up_ref, pre3_ref, stat3_ref, stat3b_ref, gs3_ref, w_ref, pre2_ref, stat2_ref, gs2_ref, g3_ref, back_ref, stat_ref):
    step = pl.program_id(0)
    rows = up_ref.shape[0]
    centre, inverse = moments(stat3_ref, 0, 4, number)
    shift_mean = unpack(stat3b_ref, 0, 4) / number
    gain_mean = unpack(stat3b_ref, 4, 4) / number
    scaled = (pre3_ref[...] - centre) * inverse
    g = gs3_ref[0:1, :] * inverse * (up_ref[...] - shift_mean - scaled * gain_mean)
    g = jnp.where(real_rows(rows), g, 0.0).astype(BF16)
    g3_ref[...] = g
    product = jnp.dot(g, w_ref[...], preferred_element_type=F32)

    @pl.when(step == 0)
    def _():
        back_ref[...] = product

    @pl.when(step > 0)
    def _():
        back_ref[...] += product

    @pl.when(step == pl.num_programs(0) - 1)
    def _():
        finish_back(number, pre2_ref, stat2_ref, gs2_ref, back_ref, stat_ref)


def finish_back(number, pre_ref, stat_in_ref, gs_ref, back_ref, stat_ref):
    rows = back_ref.shape[0]
    centre, inverse = moments(stat_in_ref, 0, 4, number)
    scaled = (pre_ref[...] - centre) * inverse
    v = gs_ref[0:1, :] * scaled + gs_ref[1:2, :]
    back = jnp.where(real_rows(rows), back_ref[...] * slope(v), 0.0)
    back_ref[...] = back
    pack(stat_ref, 0, column_sum(back))
    pack(stat_ref, 4, column_sum(back * scaled))


def normed_grad(number, back_ref, pre_ref, stat_ref, statb_ref, gs_ref):
    centre, inverse = moments(stat_ref, 0, 4, number)
    shift_mean = unpack(statb_ref, 0, 4) / number
    gain_mean = unpack(statb_ref, 4, 4) / number
    scaled = (pre_ref[...] - centre) * inverse
    g = gs_ref[0:1, :] * inverse * (back_ref[...] - shift_mean - scaled * gain_mean)
    return jnp.where(real_rows(back_ref.shape[0]), g, 0.0)


def back_one_kernel(number, back2_ref, pre2_ref, stat2_ref, stat2b_ref, gs2_ref, w_ref, pre1_ref, stat1_ref, gs1_ref, g2_ref, back_ref, stat_ref, shifted):
    step = pl.program_id(0)
    rows = back_ref.shape[0]

    @pl.when(step == 0)
    def _():
        g = normed_grad(number, back2_ref, pre2_ref, stat2_ref, stat2b_ref, gs2_ref)
        g2_ref[...] = g.astype(BF16)
        fill_shifted(shifted, g)

    piece = shifted[2 - lax.rem(step, 3), :, pl.ds(2 - lax.div(step, 3), 7)]
    piece = piece.reshape(rows, piece.shape[3]).astype(BF16)
    product = lax.dot_general(
        piece, w_ref[...], (((1,), (1,)), ((), ())), preferred_element_type=F32
    )

    @pl.when(step == 0)
    def _():
        back_ref[...] = product

    @pl.when(step > 0)
    def _():
        back_ref[...] += product

    @pl.when(step == pl.num_programs(0) - 1)
    def _():
        finish_back(number, pre1_ref, stat1_ref, gs1_ref, back_ref, stat_ref)


def grad_one_kernel(number, back_ref, pre_ref, stat_ref, statb_ref, gs_ref, g_ref):
    g_ref[...] = normed_grad(number, back_ref, pre_ref, stat_ref, statb_ref, gs_ref).astype(BF16)


def in_grad_kernel(g1_ref, w_ref, up_ref, out_ref):
    product = lax.dot_general(
        g1_ref[...], w_ref[...], (((1,), (1,)), ((), ())), preferred_element_type=F32
    )
    out_ref[...] = (up_ref[...] + product).astype(BF16).reshape(out_ref.shape)


def weight_kernel(units, table_ref, order_ref, g_ref, r_ref, out_ref, left):
    step = pl.program_id(0)

    @pl.when(step == 0)
    def _():
        t = g_ref[...].astype(F32).T.astype(BF16)
        blocks = out_ref.shape[0] // 32
        left_rows = [t[32 * k : 32 * (k + 1), :] for k in range(blocks)]
        for k in range(blocks):
            left[pl.ds(pl.multiple_of(order_ref[k] * 32, 32), 32), :] = left_rows[k]

    right = jnp.concatenate(
        [
            r_ref[:, pl.ds(pl.multiple_of(table_ref[units * step + k] * LANES, LANES), LANES)]
            for k in range(units)
        ],
        axis=1,
    )
    out_ref[...] = jnp.dot(left[...], right, preferred_element_type=F32)


def weight_part(units, table, order, g, r):
    rows, cols = g.shape
    count = table.shape[0]
    wide = r.shape[1]
    return call(
        functools.partial(weight_kernel, units),
        (count // units,),
        [whole((rows, cols)), whole((rows, wide))],
        pl.BlockSpec((cols, units * LANES), lambda i, *_: (0, i)),
        jax.ShapeDtypeStruct((cols, count * LANES), F32),
        2 * rows * cols * count * LANES,
        30,
        [pltpu.VMEM((cols, rows), BF16)],
        prefetch=2,
    )(table, order, g, r)


PAIR = {"a": [(0, 1), (1, 0), (2, 3), (3, 2)], "b": [(0, 3), (3, 0), (1, 2), (2, 1)]}
ROUTES = ((0, 1, 2, 3), (1, 2, 3, 0), (2, 3, 0, 1), (3, 0, 1, 2))
LINK = ((REP[0], "a"), (REP[0], "b"), (REP[1], "a"), (REP[1], "b"))


def of_group(stat):
    return lax.all_to_all(stat, BNGROUP, 0, 0, tiled=True)


def weight_reduced(send, keep):
    length = send.shape[1]
    got = lax.ppermute(send, BNGROUP[1], [(0, 1), (1, 0)])
    held = (keep + got).reshape(2, 2, 2, 2, 4, 8, length)
    parts = [held[:, :, :, :, k] for k in range(4)]
    live = [[0, 1, 2, 3] for _ in range(4)]
    for turn in range(4):
        for k in range(4):
            bit = ROUTES[k][turn]
            at = live[k].index(bit)
            live[k].remove(bit)
            away = lax.index_in_dim(parts[k], 1, at, keepdims=False)
            mine = lax.index_in_dim(parts[k], 0, at, keepdims=False)
            axis, kind = LINK[bit]
            parts[k] = mine + lax.ppermute(away, axis, PAIR[kind])
    return jnp.concatenate(parts, axis=0)


def per_device(images, cotangent, w_reduce, w_spatial, w_expand, norm_gain, norm_shift):
    n_img, side, _, wide = images.shape
    mid = w_reduce.shape[1]
    group_size = lax.axis_size(BNGROUP)
    images_total = n_img * group_size * lax.axis_size(REP)
    number = float(n_img * side * side * group_size)
    rows = n_img * side * 8
    step_img = 4
    steps = n_img // step_img
    step_rows = step_img * side * 8
    gs = jnp.stack([norm_gain, norm_shift])
    gs1, gs2, gs3 = gs[:, :mid], gs[:, mid : 2 * mid], gs[:, 2 * mid :]
    stat = jax.ShapeDtypeStruct((group_size, 8, LANES), F32)
    stat_spec = whole(stat.shape)
    wide_stat = jax.ShapeDtypeStruct((group_size, 32, LANES), F32)
    mid_f32 = jax.ShapeDtypeStruct((rows, mid), F32)
    mid_bf16 = jax.ShapeDtypeStruct((rows, mid), BF16)
    mid_spec = whole((rows, mid))
    gs_spec = whole((2, mid))
    image_spec = pl.BlockSpec((step_img, side, 8, wide), lambda i: (i, 0, 0, 0))
    image_shape = jax.ShapeDtypeStruct(images.shape, BF16)
    work = 2 * rows * mid * wide

    pre1, padded, stat1 = call(
        reduce_kernel,
        (steps,),
        [image_spec, whole((wide, mid))],
        [
            pl.BlockSpec((step_rows, mid), lambda i: (i, 0)),
            pl.BlockSpec((step_rows, wide), lambda i: (i, 0)),
            stat_spec,
        ],
        [mid_f32, jax.ShapeDtypeStruct((rows, wide), BF16), stat],
        work,
        24,
        [pltpu.VMEM((8, mid), F32)],
    )(images, w_reduce)
    stat1 = of_group(stat1)

    tap_spec = pl.BlockSpec((mid, mid), lambda t: (t, 0))
    shifted = pltpu.VMEM((3, n_img, 9, 8, mid), F32)
    patches, pre2, stat2 = call(
        functools.partial(conv_kernel, number),
        (9,),
        [mid_spec, stat_spec, gs_spec, tap_spec],
        [pl.BlockSpec((rows, mid), lambda t: (0, t)), mid_spec, stat_spec],
        [jax.ShapeDtypeStruct((rows, 9 * mid), BF16), mid_f32, stat],
        9 * 2 * rows * mid * mid,
        28,
        [shifted],
    )(pre1, stat1, gs1, w_spatial)
    stat2 = of_group(stat2)

    col_spec = pl.BlockSpec((rows, mid), lambda j: (0, j))
    row_spec = pl.BlockSpec((mid, mid), lambda j: (j, 0))
    stat_col_spec = pl.BlockSpec((group_size, 8, LANES), lambda j: (0, j, 0))
    hidden2, pre3, stat3 = call(
        functools.partial(expand_kernel, number),
        (wide // mid,),
        [mid_spec, stat_spec, gs_spec, row_spec],
        [mid_spec, col_spec, stat_col_spec],
        [mid_bf16, jax.ShapeDtypeStruct((rows, wide), F32), wide_stat],
        work,
        24,
    )(pre2, stat2, gs2, w_expand)
    stat3 = of_group(stat3)

    row_block = pl.BlockSpec((step_rows, wide), lambda i: (i, 0))
    output, up, stat3b = call(
        functools.partial(out_kernel, number),
        (steps,),
        [row_block, image_spec, image_spec, whole(wide_stat.shape), whole((2, wide))],
        [image_spec, row_block, whole(wide_stat.shape)],
        [image_shape, jax.ShapeDtypeStruct((rows, wide), F32), wide_stat],
        work,
        28,
        [pltpu.VMEM((16, wide), F32), pltpu.VMEM((8, wide), F32)],
    )(pre3, images, cotangent, stat3, gs3)
    stat3b = of_group(stat3b)

    grad3, back2, stat2b = call(
        functools.partial(back_two_kernel, number),
        (wide // mid,),
        [
            col_spec,
            col_spec,
            stat_col_spec,
            stat_col_spec,
            pl.BlockSpec((2, mid), lambda j: (0, j)),
            row_spec,
            mid_spec,
            stat_spec,
            gs_spec,
        ],
        [col_spec, mid_spec, stat_spec],
        [jax.ShapeDtypeStruct((rows, wide), BF16), mid_f32, stat],
        work,
        28,
    )(up, pre3, stat3, stat3b, gs3, w_expand, pre2, stat2, gs2)
    stat2b = of_group(stat2b)

    grad2, back1, stat1b = call(
        functools.partial(back_one_kernel, number),
        (9,),
        [mid_spec, mid_spec, stat_spec, stat_spec, gs_spec, tap_spec, mid_spec, stat_spec, gs_spec],
        [mid_spec, mid_spec, stat_spec],
        [mid_bf16, mid_f32, stat],
        9 * 2 * rows * mid * mid,
        32,
        [shifted],
    )(back2, pre2, stat2, stat2b, gs2, w_spatial, pre1, stat1, gs1)
    stat1b = of_group(stat1b)

    grad1 = call(
        functools.partial(grad_one_kernel, number),
        (1,),
        [mid_spec, mid_spec, stat_spec, stat_spec, gs_spec],
        mid_spec,
        mid_bf16,
        rows * mid * 40,
        16,
    )(back1, pre1, stat1, stat1b, gs1)

    core = lax.axis_index(BNGROUP[1])
    edge = jnp.array([list(range(9)), list(range(7, 16))], jnp.int32)
    taps = jnp.array(
        [
            list(range(1, 10)) + list(range(18, 27)) + [35, 35],
            list(range(9, 18)) + list(range(26, 35)) + [0, 0],
        ],
        jnp.int32,
    )
    x_at, y_at = lax.axis_index(REP[0]), lax.axis_index(REP[1])
    place = jnp.arange(16, dtype=jnp.int32)

    def bits(rel):
        b = rel >> 1
        return ((rel & 1) ^ b) * 2 + b

    order = bits((place >> 2) ^ x_at) * 4 + bits((place & 3) ^ y_at)

    def reduced(units, tables, g, r):
        send = weight_part(units, tables[1 - core], order, g, r)
        keep = weight_part(units, tables[core], order, g, r)
        return weight_reduced(send, keep)

    got_expand = reduced(3, edge, hidden2, grad3)

    def expand_side():
        return got_expand

    got_spatial = reduced(4, taps, grad2, patches)
    got_reduce = reduced(3, edge, grad1, padded)

    in_grad = call(
        in_grad_kernel,
        (steps,),
        [pl.BlockSpec((step_rows, mid), lambda i: (i, 0)), whole((wide, mid)), row_block],
        image_spec,
        image_shape,
        work,
        24,
    )(grad1, w_reduce, up)

    span = 9 * LANES
    extra = got_spatial[:, 2 * span : 2 * span + LANES]
    pad = jnp.zeros_like(extra)
    blocks = jnp.stack(
        [
            jnp.concatenate([got_reduce, extra], axis=1),
            jnp.concatenate([got_spatial[:, :span], pad], axis=1),
            jnp.concatenate([got_spatial[:, span : 2 * span], pad], axis=1),
            jnp.concatenate([extra, got_expand], axis=1),
        ]
    )
    summed = jnp.sum(lax.all_to_all(blocks, BNGROUP[0], 0, 0, tiled=True), axis=0)
    member = lax.axis_index(BNGROUP)
    offset = jnp.array([0, 192, 0, 64, 0, 64, 0, 192], jnp.int32)[member]
    mine = lax.dynamic_slice(summed, (0, offset), (summed.shape[0], 1088))
    weight_grads = mine.T / images_total

    def in_order(stat_b):
        total = jnp.sum(stat_b, axis=0).reshape(-1, 2, 4 * LANES)
        return total[:, 1].reshape(-1), total[:, 0].reshape(-1)

    sums = [in_order(s) for s in (stat1b, stat2b, stat3b)]
    group_norms = jnp.stack([jnp.concatenate([s[i] for s in sums]) for i in range(2)])
    packed = group_norms.reshape(1, -1, LANES)
    everyone = lax.all_to_all(
        jnp.broadcast_to(packed, (16,) + packed.shape[1:]), REP, 0, 0, tiled=True
    )
    norm_grads = jnp.sum(everyone, axis=0).reshape(2, -1) / images_total
    return output, in_grad, weight_grads, norm_grads


def solution(mesh):
    split = Mesh(mesh.devices.reshape(4, 2, 4, 4), BNGROUP_REP)
    data = P(BNGROUP_REP, None, None, None)
    return jax.shard_map(
        per_device,
        mesh=split,
        in_specs=(data, data, P(), P(), P(), P(), P()),
        out_specs=(data, data, P(BNGROUP, REP), P()),
        check_vma=False,
    )
```

```python
import functools

import jax
import jax.numpy as jnp
from jax import lax
from jax.experimental import pallas as pl
from jax.experimental.pallas import tpu as pltpu
from jax.sharding import Mesh
from jax.sharding import PartitionSpec as P

BNGROUP = ("bngroup_0", "bngroup_1")
REP = ("rep_0", "rep_1")
BNGROUP_REP = ("bngroup_0", "bngroup_1", "rep_0", "rep_1")
EPS = 0.25
F32 = jnp.float32
BF16 = jnp.bfloat16
MIB = 1 << 20
LANES = 128


def sigmoid(v):
    return 0.5 + 0.5 * jnp.tanh(0.5 * v)


def slope(v):
    s = sigmoid(v)
    return s * (1.0 + v * (1.0 - s))


def real_rows(rows):
    return (lax.broadcasted_iota(jnp.int32, (rows, 1), 0) & 7) != 7


def unpack(stat_ref, first, count):
    total = jnp.sum(stat_ref[:, first : first + count, :], axis=0)
    return jnp.concatenate([total[k : k + 1, :] for k in range(count)], axis=1)


def pack(out_ref, first, row):
    count = row.shape[1] // LANES
    rows = jnp.concatenate([row[:, k * LANES : (k + 1) * LANES] for k in range(count)], axis=0)
    out_ref[:, first : first + count, :] = jnp.broadcast_to(
        rows[None], (out_ref.shape[0], count, LANES)
    )


def moments(stat_ref, first, count, number):
    centre = unpack(stat_ref, first, count) / number
    second = unpack(stat_ref, first + count, count) / number
    spread = jnp.maximum(second - centre * centre, 0.0)
    return centre, lax.rsqrt(spread + EPS)


def column_sum(v):
    return jnp.sum(v, axis=0, keepdims=True)


def call(vmem, kernel, grid, in_specs, out_specs, out_shape, flops, scratch=(), prefetch=0):
    return pl.pallas_call(
        kernel,
        grid_spec=pltpu.PrefetchScalarGridSpec(
            num_scalar_prefetch=prefetch,
            grid=grid,
            in_specs=in_specs,
            out_specs=out_specs,
            scratch_shapes=list(scratch),
        ),
        out_shape=out_shape,
        compiler_params=pltpu.CompilerParams(
            dimension_semantics=("arbitrary",) * len(grid), vmem_limit_bytes=vmem * MIB
        ),
        cost_estimate=pl.CostEstimate(flops=flops, bytes_accessed=flops // 400, transcendentals=0),
    )


def whole(shape):
    return pl.BlockSpec(shape, lambda *_: (0,) * len(shape))


def reduce_kernel(x_ref, w_ref, pre_ref, xp_ref, stat_ref, sums):
    step = pl.program_id(0)
    rows = pre_ref.shape[0]
    x = x_ref[...].astype(F32).reshape(rows, x_ref.shape[3])
    x = jnp.where(real_rows(rows), x, 0.0).astype(BF16)
    xp_ref[...] = x
    p = jnp.dot(x, w_ref[...], preferred_element_type=F32)
    pre_ref[...] = p

    @pl.when(step == 0)
    def _():
        sums[...] = jnp.zeros_like(sums)

    sums[0:1, :] += column_sum(p)
    sums[1:2, :] += column_sum(p * p)

    @pl.when(step == pl.num_programs(0) - 1)
    def _():
        pack(stat_ref, 0, sums[0:1, :])
        pack(stat_ref, 4, sums[1:2, :])


def fill_shifted(shifted, field):
    images, _, _, channels = shifted.shape[1:]
    zero = jnp.zeros((images, 1, 8, channels), F32)
    rows = field.shape[0]
    for k, moved in enumerate((pltpu.roll(field, 1, 0), field, pltpu.roll(field, rows - 1, 0))):
        shifted[k, :, 1:8] = moved.reshape(images, 7, 8, channels)
        shifted[k, :, 0:1] = zero
        shifted[k, :, 8:9] = zero


def conv_kernel(number, pre1_ref, stat1_ref, gs_ref, w_ref, patch_ref, pre2_ref, stat_ref, shifted):
    step = pl.program_id(0)
    rows = pre2_ref.shape[0]

    @pl.when(step == 0)
    def _():
        centre, inverse = moments(stat1_ref, 0, 4, number)
        v = gs_ref[0:1, :] * ((pre1_ref[...] - centre) * inverse) + gs_ref[1:2, :]
        fill_shifted(shifted, jnp.where(real_rows(rows), v * sigmoid(v), 0.0))

    piece = shifted[lax.rem(step, 3), :, pl.ds(lax.div(step, 3), 7)]
    piece = piece.reshape(rows, piece.shape[3]).astype(BF16)
    patch_ref[...] = piece
    product = jnp.dot(piece, w_ref[...], preferred_element_type=F32)

    @pl.when(step == 0)
    def _():
        pre2_ref[...] = product

    @pl.when(step > 0)
    def _():
        pre2_ref[...] += product

    @pl.when(step == pl.num_programs(0) - 1)
    def _():
        p = jnp.where(real_rows(rows), pre2_ref[...], 0.0)
        pre2_ref[...] = p
        pack(stat_ref, 0, column_sum(p))
        pack(stat_ref, 4, column_sum(p * p))


def expand_kernel(number, pre2_ref, stat2_ref, gs_ref, w_ref, h2_ref, pre3_ref, stat_ref):
    rows = h2_ref.shape[0]

    @pl.when(pl.program_id(0) == 0)
    def _():
        centre, inverse = moments(stat2_ref, 0, 4, number)
        v = gs_ref[0:1, :] * ((pre2_ref[...] - centre) * inverse) + gs_ref[1:2, :]
        h2_ref[...] = jnp.where(real_rows(rows), v * sigmoid(v), 0.0).astype(BF16)

    p = lax.dot_general(
        h2_ref[...], w_ref[...], (((1,), (1,)), ((), ())), preferred_element_type=F32
    )
    pre3_ref[...] = p
    pack(stat_ref, 0, column_sum(p))
    pack(stat_ref, 4, column_sum(p * p))


def wide_moments(stat_ref, number):
    parts = [moments(stat_ref, 8 * k, 4, number) for k in range(stat_ref.shape[1] // 8)]
    return tuple(jnp.concatenate([p[i] for p in parts], axis=1) for i in range(2))


def out_kernel(number, pre3_ref, x_ref, ct_ref, stat3_ref, gs_ref, out_ref, up_ref, stat_ref, sums, rowsc):
    step = pl.program_id(0)
    images = x_ref.shape[0]

    @pl.when(step == 0)
    def _():
        centre, inverse = wide_moments(stat3_ref, number)
        rowsc[0:1, :] = centre
        rowsc[1:2, :] = inverse
        sums[...] = jnp.zeros_like(sums)

    width = 512
    real = lax.broadcasted_iota(jnp.int32, (8, width), 0) != 7
    for block in range(x_ref.shape[3] // width):
        cols = slice(block * width, (block + 1) * width)
        centre = rowsc[0:1, cols]
        inverse = rowsc[1:2, cols]
        gain = gs_ref[0:1, cols]
        shift = gs_ref[1:2, cols]

        def group(g, carry, cols=cols, centre=centre, inverse=inverse, gain=gain, shift=shift):
            first, second = carry
            image = lax.div(g, 7)
            line = lax.rem(g, 7)
            at = pl.ds(pl.multiple_of(g * 8, 8), 8)
            scaled = (pre3_ref[at, cols] - centre) * inverse
            v = gain * scaled + shift + x_ref[image, line, :, cols].astype(F32)
            s = sigmoid(v)
            out = v * s
            out_ref[image, line, :, cols] = out.astype(BF16)
            up = ct_ref[image, line, :, cols].astype(F32) * (s * (1.0 + (v - out)))
            up = jnp.where(real, up, 0.0)
            up_ref[at, cols] = up
            return first + up, second + up * scaled

        zero = jnp.zeros((8, width), F32)
        first, second = lax.fori_loop(0, images * 7, group, (zero, zero), unroll=4)
        sums[0:8, cols] += first
        sums[8:16, cols] += second

    @pl.when(step == pl.num_programs(0) - 1)
    def _():
        for k in range(stat_ref.shape[1] // 8):
            cols = slice(512 * k, 512 * (k + 1))
            pack(stat_ref, 8 * k, column_sum(sums[0:8, cols]))
            pack(stat_ref, 8 * k + 4, column_sum(sums[8:16, cols]))


def back_two_kernel(number, up_ref, pre3_ref, stat3_ref, stat3b_ref, gs3_ref, w_ref, pre2_ref, stat2_ref, gs2_ref, g3_ref, back_ref, stat_ref):
    step = pl.program_id(0)
    rows = up_ref.shape[0]
    centre, inverse = moments(stat3_ref, 0, 4, number)
    shift_mean = unpack(stat3b_ref, 0, 4) / number
    gain_mean = unpack(stat3b_ref, 4, 4) / number
    scaled = (pre3_ref[...] - centre) * inverse
    g = gs3_ref[0:1, :] * inverse * (up_ref[...] - shift_mean - scaled * gain_mean)
    g = jnp.where(real_rows(rows), g, 0.0).astype(BF16)
    g3_ref[...] = g
    product = jnp.dot(g, w_ref[...], preferred_element_type=F32)

    @pl.when(step == 0)
    def _():
        back_ref[...] = product

    @pl.when(step > 0)
    def _():
        back_ref[...] += product

    @pl.when(step == pl.num_programs(0) - 1)
    def _():
        finish_back(number, pre2_ref, stat2_ref, gs2_ref, back_ref, stat_ref)


def finish_back(number, pre_ref, stat_in_ref, gs_ref, back_ref, stat_ref):
    rows = back_ref.shape[0]
    centre, inverse = moments(stat_in_ref, 0, 4, number)
    scaled = (pre_ref[...] - centre) * inverse
    v = gs_ref[0:1, :] * scaled + gs_ref[1:2, :]
    back = jnp.where(real_rows(rows), back_ref[...] * slope(v), 0.0)
    back_ref[...] = back
    pack(stat_ref, 0, column_sum(back))
    pack(stat_ref, 4, column_sum(back * scaled))


def normed_grad(number, back_ref, pre_ref, stat_ref, statb_ref, gs_ref):
    centre, inverse = moments(stat_ref, 0, 4, number)
    shift_mean = unpack(statb_ref, 0, 4) / number
    gain_mean = unpack(statb_ref, 4, 4) / number
    scaled = (pre_ref[...] - centre) * inverse
    g = gs_ref[0:1, :] * inverse * (back_ref[...] - shift_mean - scaled * gain_mean)
    return jnp.where(real_rows(back_ref.shape[0]), g, 0.0)


def back_one_kernel(number, g2_ref, w_ref, pre1_ref, stat1_ref, gs1_ref, back_ref, stat_ref, shifted):
    step = pl.program_id(0)
    rows = back_ref.shape[0]

    @pl.when(step == 0)
    def _():
        fill_shifted(shifted, g2_ref[...].astype(F32))

    piece = shifted[2 - lax.rem(step, 3), :, pl.ds(2 - lax.div(step, 3), 7)]
    piece = piece.reshape(rows, piece.shape[3]).astype(BF16)
    product = lax.dot_general(
        piece, w_ref[...], (((1,), (1,)), ((), ())), preferred_element_type=F32
    )

    @pl.when(step == 0)
    def _():
        back_ref[...] = product

    @pl.when(step > 0)
    def _():
        back_ref[...] += product

    @pl.when(step == pl.num_programs(0) - 1)
    def _():
        finish_back(number, pre1_ref, stat1_ref, gs1_ref, back_ref, stat_ref)


def grad_one_kernel(number, back_ref, pre_ref, stat_ref, statb_ref, gs_ref, g_ref):
    g_ref[...] = normed_grad(number, back_ref, pre_ref, stat_ref, statb_ref, gs_ref).astype(BF16)


def in_grad_kernel(g1_ref, w_ref, up_ref, out_ref):
    product = lax.dot_general(
        g1_ref[...], w_ref[...], (((1,), (1,)), ((), ())), preferred_element_type=F32
    )
    out_ref[...] = (up_ref[...] + product).astype(BF16).reshape(out_ref.shape)


def picked(units, table_ref, r_ref):
    step = pl.program_id(0)
    return jnp.concatenate(
        [
            r_ref[:, pl.ds(pl.multiple_of(table_ref[units * step + k] * LANES, LANES), LANES)]
            for k in range(units)
        ],
        axis=1,
    )


def send_kernel(units, table_ref, place_ref, g_ref, r_ref, out_ref, left_ref, turned):
    @pl.when(pl.program_id(0) == 0)
    def _():
        turned[...] = g_ref[...].astype(F32).T
        for k in range(left_ref.shape[0] // 16):
            pair = [
                turned[pl.ds(pl.multiple_of(place_ref[2 * k + i] * 8, 8), 8), :] for i in range(2)
            ]
            left_ref[16 * k : 16 * (k + 1), :] = jnp.concatenate(pair, axis=0).astype(BF16)

    out_ref[...] = jnp.dot(
        left_ref[...], picked(units, table_ref, r_ref), preferred_element_type=F32
    )


def keep_kernel(units, table_ref, left_ref, r_ref, out_ref):
    out_ref[...] = jnp.dot(
        left_ref[...], picked(units, table_ref, r_ref), preferred_element_type=F32
    )


def weight_send(units, table, place, g, r):
    rows, cols = g.shape
    count = table.shape[0]
    return call(
        26,
        functools.partial(send_kernel, units),
        (count // units,),
        [whole(g.shape), whole(r.shape)],
        [pl.BlockSpec((cols, units * LANES), lambda i, *_: (0, i)), whole((cols, rows))],
        [
            jax.ShapeDtypeStruct((cols, count * LANES), F32),
            jax.ShapeDtypeStruct((cols, rows), BF16),
        ],
        2 * rows * cols * count * LANES,
        [pltpu.VMEM((cols, rows), F32)],
        prefetch=2,
    )(table, place, g, r)


def weight_keep(units, table, left, r):
    cols, rows = left.shape
    count = table.shape[0]
    return call(
        22,
        functools.partial(keep_kernel, units),
        (count // units,),
        [whole(left.shape), whole(r.shape)],
        pl.BlockSpec((cols, units * LANES), lambda i, *_: (0, i)),
        jax.ShapeDtypeStruct((cols, count * LANES), F32),
        2 * rows * cols * count * LANES,
        prefetch=1,
    )(table, left, r)


def split_kernel(keep_ref, got_ref, *out_refs):
    half = out_refs[0].shape[0]
    for k in range(4):
        for side in range(2):
            at = slice((2 * k + side) * half, (2 * k + side + 1) * half)
            out_refs[4 * side + k][...] = keep_ref[at, :] + got_ref[at, :]


def split(keep, got):
    rows, length = keep.shape
    shape = jax.ShapeDtypeStruct((rows // 8, length), F32)
    outs = call(
        36 if length > 2000 else 18,
        split_kernel,
        (1,),
        [whole(keep.shape)] * 2,
        [whole(shape.shape)] * 8,
        [shape] * 8,
        keep.size,
    )(keep, got)
    return outs[:4], outs[4:]


def turn_kernel(widths, *refs):
    count = len(widths)
    ins, outs = refs[: 8 * count + 2], refs[8 * count + 2 :]
    half = outs[0].shape[0]
    for k in range(4):
        for side in range(2):
            at = slice(side * half, (side + 1) * half)
            begin = 0
            for part, width in enumerate(widths):
                mine, got = ins[8 * part + k], ins[8 * part + 4 + k]
                outs[4 * side + k][:, begin : begin + width] = mine[at, :] + got[at, :]
                begin += width
    outs[8][...] = ins[-2][...] + ins[-1][...]


def turned(parts, norms):
    widths = tuple(mine[0].shape[1] for mine, _ in parts)
    ins = [a for mine, got in parts for a in (*mine, *got)] + list(norms)
    shape = jax.ShapeDtypeStruct((parts[0][0][0].shape[0] // 2, sum(widths)), F32)
    norm = jax.ShapeDtypeStruct(norms[0].shape, F32)
    outs = call(
        40 if shape.shape[0] == 32 else 24,
        functools.partial(turn_kernel, widths),
        (1,),
        [whole(a.shape) for a in ins],
        [whole(shape.shape)] * 8 + [whole(norm.shape)],
        [shape] * 8 + [norm],
        8 * shape.size,
    )(*ins)
    return outs[:4], outs[4:8], outs[8]


def last_kernel(spans, scale, *refs):
    mine, got, norm_ref, norm_got_ref, blocks_ref, norm_out_ref = (
        refs[:4],
        refs[4:8],
        *refs[8:],
    )
    spatial, edge = spans
    span = edge
    zero = jnp.zeros((8, LANES), F32)
    for k in range(4):
        at = slice(8 * k, 8 * (k + 1))
        total = mine[k][...] + got[k][...]
        extra = total[:, 2 * span : 2 * span + LANES]
        blocks_ref[0, at, :span] = total[:, spatial : spatial + edge]
        blocks_ref[0, at, span:] = extra
        blocks_ref[1, at, :span] = total[:, :span]
        blocks_ref[1, at, span:] = zero
        blocks_ref[2, at, :span] = total[:, span : 2 * span]
        blocks_ref[2, at, span:] = zero
        blocks_ref[3, at, :LANES] = extra
        blocks_ref[3, at, LANES:] = total[:, spatial + edge :]
    norm = (norm_ref[...] + norm_got_ref[...]) * scale
    for j in range(norm.shape[0] // 8):
        for i in range(4):
            cols = slice(512 * j + LANES * i, 512 * j + LANES * (i + 1))
            norm_out_ref[1:2, cols] = norm[8 * j + i : 8 * j + i + 1, :]
            norm_out_ref[0:1, cols] = norm[8 * j + 4 + i : 8 * j + 5 + i, :]


PAIR = {"a": [(0, 1), (1, 0), (2, 3), (3, 2)], "b": [(0, 3), (3, 0), (1, 2), (2, 1)]}
ROUTES = ((0, 1, 2, 3), (1, 2, 3, 0), (2, 3, 0, 1), (3, 0, 1, 2))
LINK = ((REP[0], "a"), (REP[0], "b"), (REP[1], "a"), (REP[1], "b"))


def add_kernel(a_ref, b_ref, out_ref):
    out_ref[...] = a_ref[...] + b_ref[...]


def added(a, b):
    spec = whole(a.shape)
    shape = jax.ShapeDtypeStruct(a.shape, F32)
    return call(2, add_kernel, (1,), [spec, spec], spec, shape, a.size)(a, b)


def of_group_in_turns(stat):
    for axis, pairs in (
        (BNGROUP[1], [(0, 1), (1, 0)]), (BNGROUP[0], PAIR["a"]), (BNGROUP[0], PAIR["b"])
    ):
        got = lax.ppermute(stat, axis, pairs)
        stat = added(stat, got)
    return stat


def core_sent(send):
    return lax.ppermute(send, BNGROUP[1], [(0, 1), (1, 0)])


def sent(turn, aways):
    got = []
    for k, away in enumerate(aways):
        axis, kind = LINK[ROUTES[k][turn]]
        got.append(lax.ppermute(away, axis, PAIR[kind]))
    return got


def per_device(images, cotangent, w_reduce, w_spatial, w_expand, norm_gain, norm_shift):
    n_img, side, _, wide = images.shape
    mid = w_reduce.shape[1]
    group_size = lax.axis_size(BNGROUP)
    images_total = n_img * group_size * lax.axis_size(REP)
    number = float(n_img * side * side * group_size)
    rows = n_img * side * 8
    step_img = 4
    steps = n_img // step_img
    step_rows = step_img * side * 8
    gs = jnp.stack([norm_gain, norm_shift])
    gs1, gs2, gs3 = gs[:, :mid], gs[:, mid : 2 * mid], gs[:, 2 * mid :]
    stat = jax.ShapeDtypeStruct((1, 8, LANES), F32)
    stat_spec = whole(stat.shape)
    wide_stat = jax.ShapeDtypeStruct((1, 32, LANES), F32)
    mid_f32 = jax.ShapeDtypeStruct((rows, mid), F32)
    mid_bf16 = jax.ShapeDtypeStruct((rows, mid), BF16)
    mid_spec = whole((rows, mid))
    gs_spec = whole((2, mid))
    image_spec = pl.BlockSpec((step_img, side, 8, wide), lambda i: (i, 0, 0, 0))
    image_shape = jax.ShapeDtypeStruct(images.shape, BF16)
    work = 2 * rows * mid * wide

    pre1, padded, stat1 = call(
        24,
        reduce_kernel,
        (steps,),
        [image_spec, whole((wide, mid))],
        [
            pl.BlockSpec((step_rows, mid), lambda i: (i, 0)),
            pl.BlockSpec((step_rows, wide), lambda i: (i, 0)),
            stat_spec,
        ],
        [mid_f32, jax.ShapeDtypeStruct((rows, wide), BF16), stat],
        work,
        [pltpu.VMEM((8, mid), F32)],
    )(images, w_reduce)
    stat1 = of_group_in_turns(stat1)

    tap_spec = pl.BlockSpec((mid, mid), lambda t: (t, 0))
    shifted = pltpu.VMEM((3, n_img, 9, 8, mid), F32)
    patches, pre2, stat2 = call(
        28,
        functools.partial(conv_kernel, number),
        (9,),
        [mid_spec, stat_spec, gs_spec, tap_spec],
        [pl.BlockSpec((rows, mid), lambda t: (0, t)), mid_spec, stat_spec],
        [jax.ShapeDtypeStruct((rows, 9 * mid), BF16), mid_f32, stat],
        9 * 2 * rows * mid * mid,
        [shifted],
    )(pre1, stat1, gs1, w_spatial)
    stat2 = of_group_in_turns(stat2)

    col_spec = pl.BlockSpec((rows, mid), lambda j: (0, j))
    row_spec = pl.BlockSpec((mid, mid), lambda j: (j, 0))
    stat_col_spec = pl.BlockSpec((1, 8, LANES), lambda j: (0, j, 0))
    hidden2, pre3, stat3 = call(
        24,
        functools.partial(expand_kernel, number),
        (wide // mid,),
        [mid_spec, stat_spec, gs_spec, row_spec],
        [mid_spec, col_spec, stat_col_spec],
        [mid_bf16, jax.ShapeDtypeStruct((rows, wide), F32), wide_stat],
        work,
    )(pre2, stat2, gs2, w_expand)
    stat3 = of_group_in_turns(stat3)

    row_block = pl.BlockSpec((step_rows, wide), lambda i: (i, 0))
    output, up, stat3b = call(
        28,
        functools.partial(out_kernel, number),
        (steps,),
        [row_block, image_spec, image_spec, whole(wide_stat.shape), whole((2, wide))],
        [image_spec, row_block, whole(wide_stat.shape)],
        [image_shape, jax.ShapeDtypeStruct((rows, wide), F32), wide_stat],
        work,
        [pltpu.VMEM((16, wide), F32), pltpu.VMEM((8, wide), F32)],
    )(pre3, images, cotangent, stat3, gs3)
    stat3b = of_group_in_turns(stat3b)

    grad3, back2, stat2b = call(
        28,
        functools.partial(back_two_kernel, number),
        (wide // mid,),
        [
            col_spec,
            col_spec,
            stat_col_spec,
            stat_col_spec,
            pl.BlockSpec((2, mid), lambda j: (0, j)),
            row_spec,
            mid_spec,
            stat_spec,
            gs_spec,
        ],
        [col_spec, mid_spec, stat_spec],
        [jax.ShapeDtypeStruct((rows, wide), BF16), mid_f32, stat],
        work,
    )(up, pre3, stat3, stat3b, gs3, w_expand, pre2, stat2, gs2)
    stat2b = of_group_in_turns(stat2b)

    def own_grad(*operands):
        return call(
            12,
            functools.partial(grad_one_kernel, number),
            (1,),
            [mid_spec, mid_spec, stat_spec, stat_spec, gs_spec],
            mid_spec,
            mid_bf16,
            rows * mid * 40,
        )(*operands)

    grad2 = own_grad(back2, pre2, stat2, stat2b, gs2)
    back1, stat1b = call(
        30,
        functools.partial(back_one_kernel, number),
        (9,),
        [mid_spec, tap_spec, mid_spec, stat_spec, gs_spec],
        [mid_spec, stat_spec],
        [mid_f32, stat],
        9 * 2 * rows * mid * mid,
        [shifted],
    )(grad2, w_spatial, pre1, stat1, gs1)
    stat1b = of_group_in_turns(stat1b)

    grad1 = own_grad(back1, pre1, stat1, stat1b, gs1)

    core = lax.axis_index(BNGROUP[1])
    edge = jnp.array([list(range(9)), list(range(7, 16))], jnp.int32)
    taps = jnp.array(
        [
            list(range(1, 10)) + list(range(18, 27)) + [35, 35],
            list(range(9, 18)) + list(range(26, 35)) + [0, 0],
        ],
        jnp.int32,
    )
    x_at, y_at = lax.axis_index(REP[0]), lax.axis_index(REP[1])
    at = jnp.arange(64, dtype=jnp.int32)
    route = at >> 4
    digit = [(at >> (3 - turn)) & 1 for turn in range(4)]
    bit = [
        sum(jnp.where(route == k, digit[ROUTES[k].index(link)], 0) for k in range(4))
        for link in range(4)
    ]
    block = (x_at ^ bit[0] ^ (3 * bit[1])) * 4 + (y_at ^ bit[2] ^ (3 * bit[3]))
    place = block * 4 + route

    def both(units, tables, g, r):
        send, left = weight_send(units, tables[1 - core], place, g, r)
        got = core_sent(send)
        keep = weight_keep(units, tables[core], left, r)
        mine, away = split(keep, got)
        return mine, sent(0, away)

    parts_e = both(3, edge, hidden2, grad3)
    parts_s = both(4, taps, grad2, patches)
    parts_r = both(3, edge, grad1, padded)

    def norm_sent(turn, value):
        axis, kind = LINK[ROUTES[0][turn]]
        return lax.ppermute(value, axis, PAIR[kind])

    norm = jnp.concatenate([s[0] for s in (stat1b, stat2b, stat3b)], axis=0)
    parts = [parts_s, parts_r, parts_e]
    for turn in (1, 2, 3):
        mine, away, norm = turned(parts, (norm, norm_sent(turn - 1, norm)))
        parts = [(mine, sent(turn, away))]
    (mine, got), = parts
    span = edge.shape[1] * LANES
    ins = [*mine, *got, norm, norm_sent(3, norm)]
    blocks_shape = (4, 32, span + LANES)
    blocks, norm_grads = call(
        8,
        functools.partial(last_kernel, (taps.shape[1] * LANES, span), 1.0 / images_total),
        (1,),
        [whole(a.shape) for a in ins],
        [whole(blocks_shape), whole((2, gs.shape[1]))],
        [jax.ShapeDtypeStruct(blocks_shape, F32), jax.ShapeDtypeStruct((2, gs.shape[1]), F32)],
        64 * span,
    )(*ins)

    in_grad = call(
        22,
        in_grad_kernel,
        (steps,),
        [pl.BlockSpec((step_rows, mid), lambda i: (i, 0)), whole((wide, mid)), row_block],
        image_spec,
        image_shape,
        work,
    )(grad1, w_reduce, up)

    summed = lax.all_to_all(blocks, BNGROUP[0], 0, 0, tiled=True)
    summed = jnp.sum(summed, axis=0)
    member = lax.axis_index(BNGROUP)
    offset = jnp.array([0, 192, 0, 64, 0, 64, 0, 192], jnp.int32)[member]
    height = 1088
    mine = jnp.where(
        offset == 0,
        summed[:, :height],
        jnp.where(offset == 64, summed[:, 64 : 64 + height], summed[:, 192:]),
    )
    return output, in_grad, mine.T / images_total, norm_grads


def solution(mesh):
    split = Mesh(mesh.devices.reshape(4, 2, 4, 4), BNGROUP_REP)
    data = P(BNGROUP_REP, None, None, None)
    return jax.shard_map(
        per_device,
        mesh=split,
        in_specs=(data, data, P(), P(), P(), P(), P()),
        out_specs=(data, data, P(BNGROUP, REP), P()),
        check_vma=False,
    )
```
